32 devices in a mesh: gx: 8 (over y, x, core), gy: 4 (over z).
Axes of the slice: x: 2, y: 2, z: 4, core: 2. Of those that a mesh axis runs over, the one named last changes fastest.
Arguments:
- node_disp: float32 [2, 256, 1024], P(None, 'gx', 'gy'), may hold values from -0.24 to 0.24
- node_vel: float32 [2, 256, 1024], P(None, 'gx', 'gy'), may hold values from -6 to 6
- node_mass: float32 [256, 1024], P('gx', 'gy'), may hold values from 0.5 to 2
- zone_mass: float32 [256, 1024], P('gx', 'gy'), may hold values from 0.5 to 2
- zone_energy: float32 [256, 1024], P('gx', 'gy'), may hold values from 0.3 to 7.5
- master_block: bfloat16 [32, 4, 1024], P(('gx', 'gy')), may hold values from -3 to 3, as said below
- owner: int32 [1], replicated, may hold values from 0 to 31
- pair_node: int32 [32, 1024], P(('gx', 'gy')), may hold values from 0 to 8191
- pair_segment: int32 [32, 1024], P(('gx', 'gy')), may hold values from 0 to 1022
- pair_side: int32 [32, 1024], P(('gx', 'gy')), may hold values 0 or 1
- pair_count: int32 [32], P(('gx', 'gy')), may hold values from 0 to 1024, as said below
Outputs:
- new_vel: float32 [2, 256, 1024], P(None, 'gx', 'gy')
- new_disp: float32 [2, 256, 1024], P(None, 'gx', 'gy')
- master_impulse: float32 [3, 1024], P(None, ('gx', 'gy'))
The draws below stay inside these ranges and needn't reach their ends.
Inputs may be any that keep to these rules, and one draw needn't show every extreme that they name: `pair_node`: local node numbers, row-major over a device's 32 x 256 block. `pair_count`: at most 1024; one device has exactly 1024 in every draw; slots at or past a device's count are not pairs. `master_block`: rows 0 and 1 lie within -0.25 to 0.25.
All inputs are finite; a program needn't handle non-finite values. No bound on the sum of `pair_side` on one device may be relied on, other than what follows from the above.
Results may differ from the reference program's by a relative error of at most 0.0015.
Values may be sent and summed in bfloat16 or wider, within the bound.
A program may use at most 128 MiB of HBM per device.

```python
import jax
import jax.numpy as jnp

CX = 32
CY = 256
MDEV = 32
PAIRS_DEV = 1024
NX = 256
NY = 1024
MNODES = 1024
N_GX = 8
N_GY = 4


def draw_zone_energy(key, part):
    row_pos = jnp.arange(NX, dtype=jnp.float32)[:, None] / NX
    col_pos = jnp.arange(NY, dtype=jnp.float32)[None, :] / NY
    level = 10.0 ** (0.5 * (row_pos + col_pos))
    factor = jnp.exp(jnp.clip(0.15 * jax.random.normal(key, (NX, NY), jnp.float32), -0.35, 0.35))
    return (0.5 * level * factor).astype(jnp.float32)


def draw_master_block(key, part):
    devices = MNODES // MDEV
    scales = jnp.array([0.08, 0.08, 1.0, 1.0], jnp.float32)[None, :, None]
    values = jax.random.truncated_normal(key, -3.0, 3.0, (devices, 4, MNODES), jnp.float32)
    return (values * scales).astype(jnp.bfloat16)


def draw_pair_segment(key, part):
    devices = MNODES // MDEV
    device_ids = jnp.arange(devices, dtype=jnp.int32)[:, None]
    offsets = jax.random.randint(jax.random.fold_in(key, 11), (devices, PAIRS_DEV), -MDEV, 2 * MDEV, dtype=jnp.int32)
    nearby = jnp.clip(device_ids * MDEV + offsets, 0, MNODES - 2)
    faraway = jax.random.randint(jax.random.fold_in(key, 12), (devices, PAIRS_DEV), 0, MNODES - 1, dtype=jnp.int32)
    picker = jax.random.randint(jax.random.fold_in(key, 13), (devices, PAIRS_DEV), 0, 2, dtype=jnp.int32)
    return jnp.where(picker == 1, faraway, nearby).astype(jnp.int32)


def draw_pair_count(key, part):
    devices = MNODES // MDEV
    first = jax.random.randint(jax.random.fold_in(key, 1), (devices,), 0, PAIRS_DEV + 1, dtype=jnp.int32)
    second = jax.random.randint(jax.random.fold_in(key, 2), (devices,), 0, PAIRS_DEV + 1, dtype=jnp.int32)
    busiest = jax.random.randint(jax.random.fold_in(key, 3), (), 0, devices, dtype=jnp.int32)
    counts = first * second // PAIRS_DEV
    return jnp.where(jnp.arange(devices, dtype=jnp.int32) == busiest, PAIRS_DEV, counts).astype(jnp.int32)


def with_ends(result, stream_key, low, top_value):
    index_at = [jax.random.randint(jax.random.fold_in(stream_key, axis), (), 0, length) for axis, length in enumerate(result.shape)]
    main_axis = result.shape.index(max(result.shape))
    beside = index_at[:main_axis] + [(index_at[main_axis] + 1) % result.shape[main_axis]] + index_at[main_axis + 1:]
    return result.at[tuple(index_at)].set(low).at[tuple(beside)].set(top_value)


def shard_levels(rng, shape, split, least, high):
    factor_of = 1.0
    for dim, blocks in split:
        heights = jax.random.uniform(jax.random.fold_in(jax.random.fold_in(rng, 6), dim), (blocks,), jnp.float32, least / len(split), high / len(split))
        factor_of = factor_of * jnp.repeat(jnp.exp(heights), shape[dim] // blocks).reshape((-1,) + (1,) * (len(shape) - 1 - dim))
    return factor_of


def bell_draw(key, dims, scale, most, pieces=(), kind=jnp.bfloat16):
    values = scale * jax.random.normal(key, dims, jnp.float32)
    if pieces:
        values = values * shard_levels(key, dims, pieces, -0.22, 0.18)
    return jnp.clip(values, -most, most).astype(kind)


def setup_inputs(seed: int = 0) -> dict:
    key_list = jax.random.split(jax.random.key(seed), 12)
    node_disp = bell_draw(key_list[0], (2, NX, NY), 0.08, 0.24, ((1, 8), (2, 4)), jnp.float32)
    node_vel = bell_draw(key_list[1], (2, NX, NY), 1.0, 6.0, ((1, 8), (2, 4)), jnp.float32)
    node_mass = jnp.clip(0.5 + 1.5 * jax.random.uniform(key_list[2], (NX, NY), jnp.float32) ** shard_levels(key_list[2], (NX, NY), ((0, 8), (1, 4)), -0.2, 0.2), 0.5, 2.0)
    zone_mass = jnp.clip(0.5 + 1.5 * jax.random.uniform(key_list[3], (NX, NY), jnp.float32) ** shard_levels(key_list[3], (NX, NY), ((0, 8), (1, 4)), -0.2, 0.2), 0.5, 2.0)
    zone_energy = draw_zone_energy(jax.random.fold_in(key_list[11], 71), 0)
    master_block = draw_master_block(jax.random.fold_in(key_list[11], 71), 0)
    owner = jax.random.randint(key_list[6], (1,), 0, N_GX * N_GY).astype(jnp.int32)
    pair_node = with_ends(jax.random.randint(key_list[7], (N_GX * N_GY, PAIRS_DEV), 0, CX * CY), jax.random.fold_in(key_list[7], 1), 0, (CX * CY) - 1).astype(jnp.int32)
    pair_segment = draw_pair_segment(jax.random.fold_in(key_list[11], 71), 0)
    pair_side = with_ends((jax.random.randint(key_list[9], (N_GX * N_GY, PAIRS_DEV), 0, 2) < 1).astype(jnp.int32), jax.random.fold_in(key_list[9], 1), 0, 1)
    pair_count = draw_pair_count(jax.random.fold_in(key_list[11], 71), 0)
    return {"node_disp": node_disp, "node_vel": node_vel, "node_mass": node_mass, "zone_mass": zone_mass, "zone_energy": zone_energy, "master_block": master_block, "owner": owner, "pair_node": pair_node, "pair_segment": pair_segment, "pair_side": pair_side, "pair_count": pair_count}


STIFFNESS = 10.0
GAP_SCALE = 0.05

def corner_forces(corner_a, corner_b, corner_c, corner_e, zone_load, zone_live):
    first_dx = 1.0 + corner_c[0] - corner_a[0]
    first_dy = 1.0 + corner_c[1] - corner_a[1]
    second_dx = -1.0 + corner_e[0] - corner_b[0]
    second_dy = 1.0 + corner_e[1] - corner_b[1]
    zone_area = 0.5 * (first_dx * second_dy - second_dx * first_dy)
    safe_area = jnp.where(zone_live, zone_area, 1.0)
    half_press = jnp.where(zone_live, 0.2 * zone_load / safe_area, 0.0)
    force_a = jnp.stack([-half_press * second_dy, half_press * second_dx])
    force_b = jnp.stack([half_press * first_dy, -half_press * first_dx])
    return (safe_area, force_a, force_b, -force_a, -force_b)

def contact_terms(slave_disp, seg_start, seg_end, side_flags, live_mask):
    rel_x = slave_disp[0] - seg_start[0] + 0.5
    rel_y = slave_disp[1] - seg_start[1]
    along_x = 1.0 + seg_end[0] - seg_start[0]
    along_y = seg_end[1] - seg_start[1]
    along_sq = along_x * along_x + along_y * along_y
    length = jnp.sqrt(along_sq)
    fraction = (rel_x * along_x + rel_y * along_y) / along_sq
    normal_x = -along_y / length
    normal_y = along_x / length
    gap_size = normal_x * rel_x + normal_y * rel_y
    side_sign = 1.0 - 2.0 * side_flags.astype(jnp.float32)
    magnitude = jnp.where(live_mask, STIFFNESS * GAP_SCALE * jax.nn.softplus(-side_sign * gap_size / GAP_SCALE), 0.0)
    slave_push = jnp.stack([magnitude * side_sign * normal_x, magnitude * side_sign * normal_y])
    react_first = jnp.stack([-(1.0 - fraction) * slave_push[0], -(1.0 - fraction) * slave_push[1], (1.0 - fraction) * magnitude])
    react_second = jnp.stack([-fraction * slave_push[0], -fraction * slave_push[1], fraction * magnitude])
    return (slave_push, react_first, react_second)

def shift_up(values, row_step, col_step):
    padded = jnp.pad(values, ((0, 0), (0, row_step), (0, col_step)))
    return padded[:, row_step:, col_step:]

def shift_down(values, row_step, col_step):
    padded = jnp.pad(values, ((0, 0), (row_step, 0), (col_step, 0)))
    return padded[:, :NX, :NY]

def reference(node_disp, node_vel, node_mass, zone_mass, zone_energy, master_block, owner, pair_node, pair_segment, pair_side, pair_count):
    row_ids = jnp.arange(NX, dtype=jnp.int32)[:, None]
    col_ids = jnp.arange(NY, dtype=jnp.int32)[None, :]
    zone_live = (row_ids < NX - 1) & (col_ids < NY - 1)
    safe_area, force_a, force_b, force_c, force_e = corner_forces(node_disp, shift_up(node_disp, 1, 0), shift_up(node_disp, 1, 1), shift_up(node_disp, 0, 1), zone_energy * zone_mass, zone_live)
    node_force = force_a + shift_down(force_b, 1, 0) + shift_down(force_c, 1, 1) + shift_down(force_e, 0, 1)
    zone_ratio = jnp.where(zone_live, jnp.sqrt(safe_area) / jnp.sqrt(0.56 * zone_energy), 1e+30)
    step_size = 0.3 * jnp.min(zone_ratio)
    surface = master_block[owner[0]].astype(jnp.float32)
    coords = surface[0:2]
    devices = N_GX * N_GY
    rows_dev = NX // N_GX
    cols_dev = NY // N_GY
    device_ids = jnp.arange(devices, dtype=jnp.int32)[:, None]
    node_row = device_ids // N_GY * rows_dev + pair_node // cols_dev
    node_col = device_ids % N_GY * cols_dev + pair_node % cols_dev
    live_mask = jnp.arange(PAIRS_DEV, dtype=jnp.int32)[None, :] < pair_count[:, None]
    slave_disp = node_disp[:, node_row, node_col]
    seg_start = jnp.take(coords, pair_segment, axis=1)
    seg_end = jnp.take(coords, pair_segment + 1, axis=1)
    slave_push, react_first, react_second = contact_terms(slave_disp, seg_start, seg_end, pair_side, live_mask)
    total_force = node_force.at[:, node_row, node_col].add(slave_push)
    reaction = jnp.zeros((3, MNODES), jnp.float32)
    reaction = reaction.at[:, pair_segment].add(react_first).at[:, pair_segment + 1].add(react_second)
    new_vel = node_vel + step_size * total_force / node_mass
    new_disp = node_disp + step_size * new_vel
    master_impulse = jnp.concatenate([surface[2:4] + step_size * reaction[0:2], step_size * reaction[2:3]], axis=0)
    return (new_vel, new_disp, master_impulse)
```

```python
import functools

import jax
import jax.numpy as jnp
from jax import lax
from jax.experimental import pallas as pl
from jax.experimental.pallas import tpu as pltpu
from jax.sharding import PartitionSpec as P

STIFFNESS = 10.0
GAP_SCALE = 0.05
MESH = pl.DeviceIdType.MESH
F32 = jnp.float32
BF16 = jnp.bfloat16


def two_parts(value):
    top = value.astype(BF16).astype(F32)
    return top, value - top


def dot_nt(left, right):
    return lax.dot_general(left, right, (((1,), (1,)), ((), ())), preferred_element_type=F32)


def rolled(value, shift, axis):
    return pltpu.roll(value, shift % value.shape[axis], axis)


def step_kernel(
    n_gx, n_gy,
    owner_ref, count_ref, disp_in, vel_in, mass_in, zmass_in, energy_in, block_in, node_in, seg_in, side_in,
    vel_out, disp_out, imp_out,
    disp, vel, mass, zmass, energy, block, node, seg, side,
    new_vel, new_disp, new_imp,
    up_pack, down_pack, left_pack, right_pack,
    from_down, from_up, from_right, from_left,
    plane_slots, line_send, line_slots, table,
    oh_col, oh_lo, oh_share, early, early_in, react, react_in,
    in_sem, out_sem, halo_send, halo_recv,
    plane_send_sem, plane_recv_sem, line_send_sem, line_recv_sem,
    early_send_sem, early_recv_sem, react_send_sem, react_recv_sem,
):
    n = n_gx * n_gy
    mx, my = lax.axis_index("gx"), lax.axis_index("gy")
    me = mx * n_gy + my
    rows, cols = disp.shape[1], disp.shape[2]
    pairs = node.shape[1]
    mnodes = block.shape[2]
    share = mnodes // n
    groups = mnodes // 128

    loads = [
        pltpu.make_async_copy(src, dst, in_sem.at[i])
        for i, (src, dst) in enumerate(
            [(block_in, block), (node_in, node), (disp_in, disp), (seg_in, seg), (energy_in, energy),
             (zmass_in, zmass), (side_in, side), (mass_in, mass), (vel_in, vel)]
        )
    ]
    for load in loads:
        load.start()
    for ref in (from_down, from_up, from_right, from_left):
        ref[...] = jnp.zeros(ref.shape, F32)

    barrier = pltpu.get_barrier_semaphore()
    for d in range(1, n_gx):
        pl.semaphore_signal(barrier, inc=1, device_id=(lax.rem(mx + d, n_gx), my), device_id_type=MESH)
    for d in range(1, n_gy):
        pl.semaphore_signal(barrier, inc=1, device_id=(mx, lax.rem(my + d, n_gy)), device_id_type=MESH)

    for load in loads[:7]:
        load.wait()

    dx, dy = disp[0], disp[1]
    zload = energy[...] * zmass[...]
    sub = lax.broadcasted_iota(jnp.int32, (8, cols), 0)
    up_pack[...] = jnp.where(sub == 0, dx[:8], jnp.where(sub == 1, rolled(dy[:8], 1, 0), 0.0))
    tail = slice(rows - 8, rows)
    down_pack[...] = jnp.where(
        sub == 7, dx[tail],
        jnp.where(sub == 6, rolled(dy[tail], -1, 0), jnp.where(sub == 5, rolled(zload[tail], -2, 0), 0.0)),
    )
    plane_slots[mx] = block[0, 0:2]

    node_id = node[...]
    seg_id = seg[...]
    seg_next = seg_id + 1
    node_row, node_col = node_id // cols, node_id % cols
    oh_col[...] = (lax.broadcasted_iota(jnp.int32, (cols, pairs), 0) == node_col).astype(F32).astype(BF16)
    oh_lo[...] = (lax.broadcasted_iota(jnp.int32, (128, pairs), 0) == seg_id % 128).astype(F32).astype(BF16)
    share_iota = lax.broadcasted_iota(jnp.int32, (n, pairs), 0)
    oh_share[:, :pairs] = (share_iota == seg_id // share).astype(F32).astype(BF16)
    oh_share[:, pairs:] = (share_iota == seg_next // share).astype(F32).astype(BF16)
    row_mask = lax.broadcasted_iota(jnp.int32, (rows, pairs), 0) == node_row

    flat = disp[...].reshape(2 * rows, cols)
    flat_top, flat_low = two_parts(flat)
    looked = jnp.dot(
        jnp.concatenate([flat_top, flat_low], axis=0).astype(BF16), oh_col[...], preferred_element_type=F32
    )
    looked = looked[: 2 * rows] + looked[2 * rows:]
    slave_x = jnp.sum(jnp.where(row_mask, looked[:rows], 0.0), axis=0, keepdims=True)
    slave_y = jnp.sum(jnp.where(row_mask, looked[rows:], 0.0), axis=0, keepdims=True)

    owner = owner_ref[0]
    master_id = lax.broadcasted_iota(jnp.int32, (1, mnodes), 1)
    prior = jnp.where(owner == me, block[0, 2:4].astype(F32), 0.0)
    prior_mask = lax.broadcasted_iota(jnp.int32, (share, mnodes), 0) == master_id % share
    prior_cols = jnp.concatenate(
        [jnp.where(prior_mask, prior[0:1], 0.0), jnp.where(prior_mask, prior[1:2], 0.0),
         jnp.zeros((128 - 2 * share, mnodes), F32)], axis=0
    ).astype(BF16)
    prior_rows = (lax.broadcasted_iota(jnp.int32, (n, mnodes), 0) == master_id // share).astype(F32).astype(BF16)
    early[...] = dot_nt(prior_rows, prior_cols)

    pl.semaphore_wait(barrier, n_gx + n_gy - 2)

    plane_copies = []
    for d in range(1, n_gx):
        plane_copies.append(pltpu.make_async_remote_copy(
            src_ref=plane_slots.at[mx], dst_ref=plane_slots.at[mx],
            send_sem=plane_send_sem.at[d], recv_sem=plane_recv_sem.at[d],
            device_id=(lax.rem(mx + d, n_gx), my), device_id_type=MESH))
        plane_copies[-1].start()

    def halo(src, dst, slot, device):
        return pltpu.make_async_remote_copy(
            src_ref=src, dst_ref=dst, send_sem=halo_send.at[slot], recv_sem=halo_recv.at[slot],
            device_id=device, device_id_type=MESH)

    to_up = halo(up_pack, from_down, 0, (jnp.maximum(mx - 1, 0), my))
    to_down = halo(down_pack, from_up, 1, (jnp.minimum(mx + 1, n_gx - 1), my))
    to_left = halo(left_pack, from_right, 2, (mx, jnp.maximum(my - 1, 0)))
    to_right = halo(right_pack, from_left, 3, (mx, jnp.minimum(my + 1, n_gy - 1)))
    has_up, has_down = mx > 0, mx < n_gx - 1
    has_left, has_right = my > 0, my < n_gy - 1

    @pl.when(has_up)
    def _():
        to_up.start()

    @pl.when(has_down)
    def _():
        to_down.start()

    @pl.when(has_down)
    def _():
        to_up.wait_recv()

    @pl.when(has_up)
    def _():
        to_down.wait_recv()

    below, above = from_down[...], from_up[...]
    ext_x = jnp.concatenate([dx, jnp.where(sub < 4, below, above)], axis=0)
    ext_y = jnp.concatenate([dy, jnp.where(sub < 4, rolled(below, -1, 0), rolled(above, 1, 0))], axis=0)
    ext_l = jnp.concatenate([zload, rolled(above, 2, 0)], axis=0)
    lane = lax.broadcasted_iota(jnp.int32, (rows + 8, 128), 1)
    last = slice(cols - 128, cols)
    left_pack[...] = jnp.where(lane == 0, ext_x[:, :128], jnp.where(lane == 1, rolled(ext_y[:, :128], 1, 1), 0.0))
    right_pack[...] = jnp.where(
        lane == 127, ext_x[:, last],
        jnp.where(lane == 126, rolled(ext_y[:, last], -1, 1),
                  jnp.where(lane == 125, rolled(ext_l[:, last], -2, 1), 0.0)),
    )

    @pl.when(has_left)
    def _():
        to_left.start()

    @pl.when(has_right)
    def _():
        to_right.start()

    for d in range(1, n_gx):
        pltpu.make_async_remote_copy(
            src_ref=plane_slots.at[mx], dst_ref=plane_slots.at[lax.rem(mx + n_gx - d, n_gx)],
            send_sem=plane_send_sem.at[d], recv_sem=plane_recv_sem.at[d],
            device_id=(lax.rem(mx + d, n_gx), my), device_id_type=MESH).wait_recv()

    line_slots[my] = plane_slots[owner // n_gy]
    line_copies = []
    for d in range(1, n_gy):
        line_copies.append(pltpu.make_async_remote_copy(
            src_ref=line_slots.at[my], dst_ref=line_slots.at[my],
            send_sem=line_send_sem.at[d], recv_sem=line_recv_sem.at[d],
            device_id=(mx, lax.rem(my + d, n_gy)), device_id_type=MESH))
        line_copies[-1].start()

    @pl.when(has_right)
    def _():
        to_left.wait_recv()

    @pl.when(has_left)
    def _():
        to_right.wait_recv()

    right, left = from_right[...], from_left[...]
    ext_x = jnp.concatenate([ext_x, jnp.where(lane < 64, right, left)], axis=1)
    ext_y = jnp.concatenate([ext_y, jnp.where(lane < 64, rolled(right, -1, 1), rolled(left, 1, 1))], axis=1)
    ext_l = jnp.concatenate([ext_l, rolled(left, 2, 1)], axis=1)
    ext_shape = ext_x.shape
    zone_row = lax.broadcasted_iota(jnp.int32, ext_shape, 0)
    zone_row = jnp.where(zone_row == ext_shape[0] - 1, -1, zone_row) + mx * rows
    zone_col = lax.broadcasted_iota(jnp.int32, ext_shape, 1)
    zone_col = jnp.where(zone_col == ext_shape[1] - 1, -1, zone_col) + my * cols
    live = (zone_row >= 0) & (zone_row < n_gx * rows - 1) & (zone_col >= 0) & (zone_col < n_gy * cols - 1)
    b_x, b_y = rolled(ext_x, -1, 0), rolled(ext_y, -1, 0)
    c_x, c_y = rolled(b_x, -1, 1), rolled(b_y, -1, 1)
    e_x, e_y = rolled(ext_x, -1, 1), rolled(ext_y, -1, 1)
    first_dx, first_dy = 1.0 + c_x - ext_x, 1.0 + c_y - ext_y
    second_dx, second_dy = -1.0 + e_x - b_x, 1.0 + e_y - b_y
    area = jnp.where(live, 0.5 * (first_dx * second_dy - second_dx * first_dy), 1.0)
    half_press = jnp.where(live, 0.2 * ext_l / area, 0.0)
    fa_x, fa_y = -half_press * second_dy, half_press * second_dx
    fb_x, fb_y = half_press * first_dy, -half_press * first_dx

    def gather_force(on_a, on_b):
        total = on_a + rolled(on_b - rolled(on_a, 1, 1), 1, 0) - rolled(on_b, 1, 1)
        return total[:rows, :cols]

    force_x, force_y = gather_force(fa_x, fb_x), gather_force(fa_y, fb_y)
    ratio = jnp.where(
        live[:rows, :cols], jnp.sqrt(area[:rows, :cols]) / jnp.sqrt(0.56 * energy[...]), 1e30
    )
    smallest = jnp.min(jnp.min(ratio, axis=0, keepdims=True), axis=1, keepdims=True)
    early_lane = lax.broadcasted_iota(jnp.int32, (n, 128), 1)
    early[...] = jnp.where(early_lane < 2 * share, early[...], smallest)

    for d in range(1, n_gy):
        pltpu.make_async_remote_copy(
            src_ref=line_slots.at[my], dst_ref=line_slots.at[lax.rem(my + n_gy - d, n_gy)],
            send_sem=line_send_sem.at[d], recv_sem=line_recv_sem.at[d],
            device_id=(mx, lax.rem(my + d, n_gy)), device_id_type=MESH).wait_recv()

    def exchange(sent, landed, send_sem, recv_sem):
        def copy(d, slot):
            target = lax.rem(me + d, n)
            return pltpu.make_async_remote_copy(
                src_ref=sent.at[pl.ds(target, 1)], dst_ref=landed.at[pl.ds(slot, 1)],
                send_sem=send_sem.at[d], recv_sem=recv_sem.at[d],
                device_id=(target // n_gy, lax.rem(target, n_gy)), device_id_type=MESH)

        def start():
            landed[pl.ds(me, 1), :] = sent[pl.ds(me, 1), :]

            def body(d, carry):
                copy(d, me).start()
                return carry
            lax.fori_loop(1, n, body, 0)

        def arrive():
            def body(d, carry):
                copy(d, lax.rem(me + n - d, n)).wait_recv()
                return carry
            lax.fori_loop(1, n, body, 0)

        def drain():
            def body(d, carry):
                copy(d, me).wait_send()
                return carry
            lax.fori_loop(1, n, body, 0)
        return start, arrive, drain

    early_start, early_arrive, early_drain = exchange(early, early_in, early_send_sem, early_recv_sem)
    react_start, react_arrive, react_drain = exchange(react, react_in, react_send_sem, react_recv_sem)
    early_start()

    coords = line_slots[lax.rem(owner, n_gy)].astype(F32)
    shifted = rolled(coords, -1, 1)
    for q, (source, comp) in enumerate([(coords, 0), (coords, 1), (shifted, 0), (shifted, 1)]):
        for h in range(groups):
            table[q * groups + h:q * groups + h + 1, :] = source[comp:comp + 1, h * 128:(h + 1) * 128]
    looked = jnp.dot(table[...].astype(BF16), oh_lo[...], preferred_element_type=F32)
    group_mask = lax.broadcasted_iota(jnp.int32, (groups, pairs), 0) == seg_id // 128
    start_x, start_y, end_x, end_y = [
        jnp.sum(jnp.where(group_mask, looked[q * groups:(q + 1) * groups], 0.0), axis=0, keepdims=True)
        for q in range(4)
    ]
    live_mask = lax.broadcasted_iota(jnp.int32, (1, pairs), 1) < count_ref[0]
    rel_x, rel_y = slave_x - start_x + 0.5, slave_y - start_y
    along_x, along_y = 1.0 + end_x - start_x, end_y - start_y
    along_sq = along_x * along_x + along_y * along_y
    length = jnp.sqrt(along_sq)
    fraction = (rel_x * along_x + rel_y * along_y) / along_sq
    normal_x, normal_y = -along_y / length, along_x / length
    gap_size = normal_x * rel_x + normal_y * rel_y
    side_sign = 1.0 - 2.0 * side[...].astype(F32)
    pressed = -side_sign * gap_size / GAP_SCALE
    soft = jnp.maximum(pressed, 0.0) + jnp.log1p(jnp.exp(-jnp.abs(pressed)))
    magnitude = jnp.where(live_mask, STIFFNESS * GAP_SCALE * soft, 0.0)
    push_x, push_y = magnitude * side_sign * normal_x, magnitude * side_sign * normal_y
    terms = (-push_x, -push_y, magnitude)
    firsts = [two_parts((1.0 - fraction) * t) for t in terms]
    seconds = [two_parts(fraction * t) for t in terms]
    lane_iota = lax.broadcasted_iota(jnp.int32, (share, pairs), 0)
    total = None
    for values, ids, half in ((firsts, seg_id, 0), (seconds, seg_next, 1)):
        lane_mask = lane_iota == ids % share
        for part in range(2):
            spread = jnp.concatenate(
                [jnp.where(lane_mask, values[c][part], 0.0) for c in range(3)]
                + [jnp.zeros((128 - 3 * share, pairs), F32)], axis=0
            ).astype(BF16)
            piece = dot_nt(oh_share[:, half * pairs:(half + 1) * pairs], spread)
            total = piece if total is None else total + piece
    react[...] = total
    react_start()

    (px_top, px_low), (py_top, py_low) = two_parts(push_x), two_parts(push_y)
    placed = jnp.concatenate(
        [jnp.where(row_mask, v, 0.0).astype(BF16) for v in (px_top, py_top, px_low, py_low)], axis=0
    )
    pushed = dot_nt(placed, oh_col[...])
    pushed = pushed[: 2 * rows] + pushed[2 * rows:]
    loads[7].wait()
    loads[8].wait()
    inv_mass = 1.0 / mass[...]
    accel_x = (force_x + pushed[:rows]) * inv_mass
    accel_y = (force_y + pushed[rows:]) * inv_mass

    early_arrive()
    landed = early_in[...]
    prior_sum = jnp.sum(landed, axis=0, keepdims=True)
    lowest = jnp.where(early_lane < 2 * share, 1e30, landed)
    step = 0.3 * jnp.min(jnp.min(lowest, axis=0, keepdims=True), axis=1, keepdims=True)
    for c, accel in enumerate((accel_x, accel_y)):
        speed = vel[c] + step * accel
        new_vel[c] = speed
        new_disp[c] = disp[c] + step * speed
    outs = [pltpu.make_async_copy(new_vel, vel_out, out_sem.at[0]),
            pltpu.make_async_copy(new_disp, disp_out, out_sem.at[1])]
    for out in outs:
        out.start()

    react_arrive()
    react_sum = step * jnp.sum(react_in[...], axis=0, keepdims=True)
    for c in range(3):
        piece = react_sum[:, c * share:(c + 1) * share]
        if c < 2:
            piece = piece + prior_sum[:, c * share:(c + 1) * share]
        new_imp[c:c + 1, :] = piece
    last_out = pltpu.make_async_copy(new_imp, imp_out, out_sem.at[2])
    last_out.start()

    for copy in plane_copies + line_copies:
        copy.wait_send()

    @pl.when(has_up)
    def _():
        to_up.wait_send()

    @pl.when(has_down)
    def _():
        to_down.wait_send()

    @pl.when(has_left)
    def _():
        to_left.wait_send()

    @pl.when(has_right)
    def _():
        to_right.wait_send()

    early_drain()
    react_drain()
    for out in outs + [last_out]:
        out.wait()


def shards(n_gx, n_gy, node_disp, node_vel, node_mass, zone_mass, zone_energy, master_block, owner,
           pair_node, pair_segment, pair_side, pair_count):
    n = n_gx * n_gy
    rows, cols = node_mass.shape
    pairs = pair_node.shape[1]
    mnodes = master_block.shape[2]
    share = mnodes // n
    any_spec = pl.BlockSpec(memory_space=pl.ANY)
    smem = pl.BlockSpec(memory_space=pltpu.SMEM)
    vm = pltpu.VMEM
    dma = pltpu.SemaphoreType.DMA
    i32 = jnp.int32
    return pl.pallas_call(
        functools.partial(step_kernel, n_gx, n_gy),
        out_shape=(
            jax.ShapeDtypeStruct((2, rows, cols), F32),
            jax.ShapeDtypeStruct((2, rows, cols), F32),
            jax.ShapeDtypeStruct((3, share), F32),
        ),
        in_specs=[smem, smem] + [any_spec] * 9,
        out_specs=(any_spec,) * 3,
        scratch_shapes=[
            vm((2, rows, cols), F32), vm((2, rows, cols), F32), vm((rows, cols), F32), vm((rows, cols), F32),
            vm((rows, cols), F32), vm((1, 4, mnodes), BF16), vm((1, pairs), i32), vm((1, pairs), i32),
            vm((1, pairs), i32),
            vm((2, rows, cols), F32), vm((2, rows, cols), F32), vm((3, share), F32),
            vm((8, cols), F32), vm((8, cols), F32), vm((rows + 8, 128), F32), vm((rows + 8, 128), F32),
            vm((8, cols), F32), vm((8, cols), F32), vm((rows + 8, 128), F32), vm((rows + 8, 128), F32),
            vm((n_gx, 2, mnodes), BF16), vm((2, mnodes), BF16), vm((n_gy, 2, mnodes), BF16),
            vm((4 * (mnodes // 128), 128), F32),
            vm((cols, pairs), BF16), vm((128, pairs), BF16), vm((n, 2 * pairs), BF16),
            vm((n, 128), F32), vm((n, 128), F32), vm((n, 128), F32), vm((n, 128), F32),
            dma((9,)), dma((3,)), dma((4,)), dma((4,)),
            dma((n_gx,)), dma((n_gx,)), dma((n_gy,)), dma((n_gy,)),
            dma((n,)), dma((n,)), dma((n,)), dma((n,)),
        ],
        compiler_params=pltpu.CompilerParams(collective_id=0, has_side_effects=True),
    )(owner, pair_count, node_disp, node_vel, node_mass, zone_mass, zone_energy, master_block,
      pair_node, pair_segment, pair_side)


def solution(mesh):
    in_specs = (
        P(None, "gx", "gy"), P(None, "gx", "gy"), P("gx", "gy"), P("gx", "gy"), P("gx", "gy"),
        P(("gx", "gy"), None, None), P(), P(("gx", "gy"), None), P(("gx", "gy"), None),
        P(("gx", "gy"), None), P(("gx", "gy")),
    )
    out_specs = (P(None, "gx", "gy"), P(None, "gx", "gy"), P(None, ("gx", "gy")))
    body = functools.partial(shards, mesh.shape["gx"], mesh.shape["gy"])
    return jax.shard_map(body, mesh=mesh, in_specs=in_specs, out_specs=out_specs, check_vma=False)
```

```python
import functools

import jax
import jax.numpy as jnp
from jax import lax
from jax.experimental import pallas as pl
from jax.experimental.pallas import tpu as pltpu
from jax.sharding import PartitionSpec as P

STIFFNESS = 10.0
GAP_SCALE = 0.05
MESH = pl.DeviceIdType.MESH
F32 = jnp.float32
BF16 = jnp.bfloat16


def two_parts(value):
    top = value.astype(BF16).astype(F32)
    return top, value - top


def dot_nt(left, right):
    return lax.dot_general(left, right, (((1,), (1,)), ((), ())), preferred_element_type=F32)


def rolled(value, shift, axis):
    return pltpu.roll(value, shift % value.shape[axis], axis)


def step_kernel(
    n_gx, n_gy,
    owner_in, count_in, disp_in, vel_in, mass_in, zmass_in, energy_in, block_in, node_in, seg_in, side_in,
    new_vel, new_disp, new_imp,
    owner_ref, count_ref, disp, vel, mass, zmass, energy, block, node, seg, side,
    up_pack, down_pack, left_pack, right_pack,
    from_down, from_up, from_right, from_left,
    plane_slots, line_slots, table,
    oh_col, oh_lo, oh_share, early, early_in, react, react_in,
    in_sem, halo_send, halo_recv,
    plane_send_sem, plane_recv_sem, line_send_sem, line_recv_sem,
    early_send_sem, early_recv_sem, react_send_sem, react_recv_sem,
):
    n = n_gx * n_gy
    mx, my = lax.axis_index("gx"), lax.axis_index("gy")
    me = mx * n_gy + my
    rows, cols = disp.shape[1], disp.shape[2]
    pairs = node.shape[1]
    mnodes = block.shape[2]
    share = mnodes // n
    groups = mnodes // 128

    loads = [
        pltpu.make_async_copy(src, dst, in_sem.at[i])
        for i, (src, dst) in enumerate(
            [(block_in, block), (node_in, node), (disp_in, disp), (seg_in, seg), (energy_in, energy),
             (zmass_in, zmass), (side_in, side), (owner_in, owner_ref), (count_in, count_ref), (mass_in, mass), (vel_in, vel)]
        )
    ]
    for load in loads:
        load.start()
    for ref in (from_down, from_up, from_right, from_left):
        ref[...] = jnp.zeros(ref.shape, F32)

    barrier = pltpu.get_barrier_semaphore()
    for d in range(1, n_gx):
        pl.semaphore_signal(barrier, inc=1, device_id=(lax.rem(mx + d, n_gx), my), device_id_type=MESH)
    for d in range(1, n_gy):
        pl.semaphore_signal(barrier, inc=1, device_id=(mx, lax.rem(my + d, n_gy)), device_id_type=MESH)

    for load in loads[:9]:
        load.wait()

    dx, dy = disp[0], disp[1]
    zload = energy[...] * zmass[...]
    sub = lax.broadcasted_iota(jnp.int32, (8, cols), 0)
    up_pack[...] = jnp.where(sub == 0, dx[:8], jnp.where(sub == 1, rolled(dy[:8], 1, 0), 0.0))
    tail = slice(rows - 8, rows)
    down_pack[...] = jnp.where(
        sub == 7, dx[tail],
        jnp.where(sub == 6, rolled(dy[tail], -1, 0), jnp.where(sub == 5, rolled(zload[tail], -2, 0), 0.0)),
    )
    own = block[0, 0:2].astype(F32)
    for c in range(2):
        for h in range(groups):
            table[c * groups + h:c * groups + h + 1, :] = own[c:c + 1, h * 128:(h + 1) * 128]
    plane_slots[mx] = table[...].astype(BF16)

    node_id = node[...]
    seg_id = seg[...]
    seg_next = seg_id + 1
    node_row, node_col = node_id // cols, node_id % cols
    oh_col[...] = (lax.broadcasted_iota(jnp.int32, (cols, pairs), 0) == node_col).astype(F32).astype(BF16)
    oh_lo[...] = (lax.broadcasted_iota(jnp.int32, (128, pairs), 0) == seg_id % 128).astype(F32).astype(BF16)
    share_iota = lax.broadcasted_iota(jnp.int32, (n, pairs), 0)
    oh_share[:, :pairs] = (share_iota == seg_id // share).astype(F32).astype(BF16)
    oh_share[:, pairs:] = (share_iota == seg_next // share).astype(F32).astype(BF16)
    row_mask = lax.broadcasted_iota(jnp.int32, (rows, pairs), 0) == node_row

    flat = disp[...].reshape(2 * rows, cols)
    flat_top, flat_low = two_parts(flat)
    looked = jnp.dot(
        jnp.concatenate([flat_top, flat_low], axis=0).astype(BF16), oh_col[...], preferred_element_type=F32
    )
    looked = looked[: 2 * rows] + looked[2 * rows:]
    slave_x = jnp.sum(jnp.where(row_mask, looked[:rows], 0.0), axis=0, keepdims=True)
    slave_y = jnp.sum(jnp.where(row_mask, looked[rows:], 0.0), axis=0, keepdims=True)

    owner = owner_ref[0]
    master_id = lax.broadcasted_iota(jnp.int32, (1, mnodes), 1)
    prior = jnp.where(owner == me, block[0, 2:4].astype(F32), 0.0)
    prior_mask = lax.broadcasted_iota(jnp.int32, (share, mnodes), 0) == master_id % share
    prior_cols = jnp.concatenate(
        [jnp.where(prior_mask, prior[0:1], 0.0), jnp.where(prior_mask, prior[1:2], 0.0),
         jnp.zeros((128 - 2 * share, mnodes), F32)], axis=0
    ).astype(BF16)
    prior_rows = (lax.broadcasted_iota(jnp.int32, (n, mnodes), 0) == master_id // share).astype(F32).astype(BF16)
    early[...] = dot_nt(prior_rows, prior_cols)

    pl.semaphore_wait(barrier, n_gx + n_gy - 2)

    plane_copies = []
    for d in range(1, n_gx):
        plane_copies.append(pltpu.make_async_remote_copy(
            src_ref=plane_slots.at[mx], dst_ref=plane_slots.at[mx],
            send_sem=plane_send_sem.at[d], recv_sem=plane_recv_sem.at[d],
            device_id=(lax.rem(mx + d, n_gx), my), device_id_type=MESH))
        plane_copies[-1].start()

    def halo(src, dst, slot, device):
        return pltpu.make_async_remote_copy(
            src_ref=src, dst_ref=dst, send_sem=halo_send.at[slot], recv_sem=halo_recv.at[slot],
            device_id=device, device_id_type=MESH)

    to_up = halo(up_pack, from_down, 0, (jnp.maximum(mx - 1, 0), my))
    to_down = halo(down_pack, from_up, 1, (jnp.minimum(mx + 1, n_gx - 1), my))
    to_left = halo(left_pack, from_right, 2, (mx, jnp.maximum(my - 1, 0)))
    to_right = halo(right_pack, from_left, 3, (mx, jnp.minimum(my + 1, n_gy - 1)))
    has_up, has_down = mx > 0, mx < n_gx - 1
    has_left, has_right = my > 0, my < n_gy - 1

    @pl.when(has_up)
    def _():
        to_up.start()

    @pl.when(has_down)
    def _():
        to_down.start()

    for d in range(1, n_gx):
        pltpu.make_async_remote_copy(
            src_ref=plane_slots.at[mx], dst_ref=plane_slots.at[lax.rem(mx + n_gx - d, n_gx)],
            send_sem=plane_send_sem.at[d], recv_sem=plane_recv_sem.at[d],
            device_id=(lax.rem(mx + d, n_gx), my), device_id_type=MESH).wait_recv()

    line_slots[my] = plane_slots[owner // n_gy]
    line_copies = []
    for d in range(1, n_gy):
        line_copies.append(pltpu.make_async_remote_copy(
            src_ref=line_slots.at[my], dst_ref=line_slots.at[my],
            send_sem=line_send_sem.at[d], recv_sem=line_recv_sem.at[d],
            device_id=(mx, lax.rem(my + d, n_gy)), device_id_type=MESH))
        line_copies[-1].start()

    @pl.when(has_down)
    def _():
        to_up.wait_recv()

    @pl.when(has_up)
    def _():
        to_down.wait_recv()

    below, above = from_down[...], from_up[...]
    ext_x = jnp.concatenate([dx, jnp.where(sub < 4, below, above)], axis=0)
    ext_y = jnp.concatenate([dy, jnp.where(sub < 4, rolled(below, -1, 0), rolled(above, 1, 0))], axis=0)
    ext_l = jnp.concatenate([zload, rolled(above, 2, 0)], axis=0)
    lane = lax.broadcasted_iota(jnp.int32, (rows + 8, 128), 1)
    last = slice(cols - 128, cols)
    left_pack[...] = jnp.where(lane == 0, ext_x[:, :128], jnp.where(lane == 1, rolled(ext_y[:, :128], 1, 1), 0.0))
    right_pack[...] = jnp.where(
        lane == 127, ext_x[:, last],
        jnp.where(lane == 126, rolled(ext_y[:, last], -1, 1),
                  jnp.where(lane == 125, rolled(ext_l[:, last], -2, 1), 0.0)),
    )

    @pl.when(has_left)
    def _():
        to_left.start()

    @pl.when(has_right)
    def _():
        to_right.start()

    @pl.when(has_right)
    def _():
        to_left.wait_recv()

    @pl.when(has_left)
    def _():
        to_right.wait_recv()

    right, left = from_right[...], from_left[...]
    ext_x = jnp.concatenate([ext_x, jnp.where(lane < 64, right, left)], axis=1)
    ext_y = jnp.concatenate([ext_y, jnp.where(lane < 64, rolled(right, -1, 1), rolled(left, 1, 1))], axis=1)
    ext_l = jnp.concatenate([ext_l, rolled(left, 2, 1)], axis=1)
    ext_shape = ext_x.shape
    zone_row = lax.broadcasted_iota(jnp.int32, ext_shape, 0)
    zone_row = jnp.where(zone_row == ext_shape[0] - 1, -1, zone_row) + mx * rows
    zone_col = lax.broadcasted_iota(jnp.int32, ext_shape, 1)
    zone_col = jnp.where(zone_col == ext_shape[1] - 1, -1, zone_col) + my * cols
    live = (zone_row >= 0) & (zone_row < n_gx * rows - 1) & (zone_col >= 0) & (zone_col < n_gy * cols - 1)
    b_x, b_y = rolled(ext_x, -1, 0), rolled(ext_y, -1, 0)
    c_x, c_y = rolled(b_x, -1, 1), rolled(b_y, -1, 1)
    e_x, e_y = rolled(ext_x, -1, 1), rolled(ext_y, -1, 1)
    first_dx, first_dy = 1.0 + c_x - ext_x, 1.0 + c_y - ext_y
    second_dx, second_dy = -1.0 + e_x - b_x, 1.0 + e_y - b_y
    area = jnp.where(live, 0.5 * (first_dx * second_dy - second_dx * first_dy), 1.0)
    half_press = jnp.where(live, 0.2 * ext_l / area, 0.0)
    fa_x, fa_y = -half_press * second_dy, half_press * second_dx
    fb_x, fb_y = half_press * first_dy, -half_press * first_dx

    def gather_force(on_a, on_b):
        total = on_a + rolled(on_b - rolled(on_a, 1, 1), 1, 0) - rolled(on_b, 1, 1)
        return total[:rows, :cols]

    force_x, force_y = gather_force(fa_x, fb_x), gather_force(fa_y, fb_y)
    ratio = jnp.where(
        live[:rows, :cols], jnp.sqrt(area[:rows, :cols]) / jnp.sqrt(0.56 * energy[...]), 1e30
    )
    smallest = jnp.min(jnp.min(ratio, axis=0, keepdims=True), axis=1, keepdims=True)
    early_lane = lax.broadcasted_iota(jnp.int32, (n, 128), 1)
    early[...] = jnp.where(early_lane < 2 * share, early[...], smallest)

    for d in range(1, n_gy):
        pltpu.make_async_remote_copy(
            src_ref=line_slots.at[my], dst_ref=line_slots.at[lax.rem(my + n_gy - d, n_gy)],
            send_sem=line_send_sem.at[d], recv_sem=line_recv_sem.at[d],
            device_id=(mx, lax.rem(my + d, n_gy)), device_id_type=MESH).wait_recv()

    def exchange(sent, landed, send_sem, recv_sem):
        def copy(d, slot):
            target = lax.rem(me + d, n)
            return pltpu.make_async_remote_copy(
                src_ref=sent.at[pl.ds(target, 1)], dst_ref=landed.at[pl.ds(slot, 1)],
                send_sem=send_sem.at[d], recv_sem=recv_sem.at[d],
                device_id=(target // n_gy, lax.rem(target, n_gy)), device_id_type=MESH)

        def start():
            landed[pl.ds(me, 1), :] = sent[pl.ds(me, 1), :]

            def body(d, carry):
                copy(d, me).start()
                return carry
            lax.fori_loop(1, n, body, 0)

        def arrive():
            def body(d, carry):
                copy(d, lax.rem(me + n - d, n)).wait_recv()
                return carry
            lax.fori_loop(1, n, body, 0)

        def drain():
            def body(d, carry):
                copy(d, me).wait_send()
                return carry
            lax.fori_loop(1, n, body, 0)
        return start, arrive, drain

    early_start, early_arrive, early_drain = exchange(early, early_in, early_send_sem, early_recv_sem)
    react_start, react_arrive, react_drain = exchange(react, react_in, react_send_sem, react_recv_sem)
    early_start()

    coords = line_slots[lax.rem(owner, n_gy)].astype(F32)
    shifted = rolled(coords, -1, 1)
    last_lane = lax.broadcasted_iota(jnp.int32, coords.shape, 1) == 127
    shifted = jnp.where(last_lane, rolled(shifted, -1, 0), shifted)
    looked = jnp.dot(
        jnp.concatenate([coords, shifted], axis=0).astype(BF16), oh_lo[...], preferred_element_type=F32
    )
    group_mask = lax.broadcasted_iota(jnp.int32, (groups, pairs), 0) == seg_id // 128
    start_x, start_y, end_x, end_y = [
        jnp.sum(jnp.where(group_mask, looked[q * groups:(q + 1) * groups], 0.0), axis=0, keepdims=True)
        for q in range(4)
    ]
    live_mask = lax.broadcasted_iota(jnp.int32, (1, pairs), 1) < count_ref[0]
    rel_x, rel_y = slave_x - start_x + 0.5, slave_y - start_y
    along_x, along_y = 1.0 + end_x - start_x, end_y - start_y
    along_sq = along_x * along_x + along_y * along_y
    length = jnp.sqrt(along_sq)
    fraction = (rel_x * along_x + rel_y * along_y) / along_sq
    normal_x, normal_y = -along_y / length, along_x / length
    gap_size = normal_x * rel_x + normal_y * rel_y
    side_sign = 1.0 - 2.0 * side[...].astype(F32)
    pressed = -side_sign * gap_size / GAP_SCALE
    soft = jnp.maximum(pressed, 0.0) + jnp.log1p(jnp.exp(-jnp.abs(pressed)))
    magnitude = jnp.where(live_mask, STIFFNESS * GAP_SCALE * soft, 0.0)
    push_x, push_y = magnitude * side_sign * normal_x, magnitude * side_sign * normal_y
    terms = (-push_x, -push_y, magnitude)
    firsts = [two_parts((1.0 - fraction) * t) for t in terms]
    seconds = [two_parts(fraction * t) for t in terms]
    lane_iota = lax.broadcasted_iota(jnp.int32, (share, pairs), 0)
    total = None
    for values, ids, half in ((firsts, seg_id, 0), (seconds, seg_next, 1)):
        lane_mask = lane_iota == ids % share
        for part in range(2):
            spread = jnp.concatenate(
                [jnp.where(lane_mask, values[c][part], 0.0) for c in range(3)]
                + [jnp.zeros((128 - 3 * share, pairs), F32)], axis=0
            ).astype(BF16)
            piece = dot_nt(oh_share[:, half * pairs:(half + 1) * pairs], spread)
            total = piece if total is None else total + piece
    react[...] = total
    react_start()

    (px_top, px_low), (py_top, py_low) = two_parts(push_x), two_parts(push_y)
    placed = jnp.concatenate(
        [jnp.where(row_mask, v, 0.0).astype(BF16) for v in (px_top, py_top, px_low, py_low)], axis=0
    )
    pushed = dot_nt(placed, oh_col[...])
    pushed = pushed[: 2 * rows] + pushed[2 * rows:]
    loads[9].wait()
    loads[10].wait()
    inv_mass = 1.0 / mass[...]
    accel_x = (force_x + pushed[:rows]) * inv_mass
    accel_y = (force_y + pushed[rows:]) * inv_mass

    early_arrive()
    landed = early_in[...]
    prior_sum = jnp.sum(landed, axis=0, keepdims=True)
    lowest = jnp.where(early_lane < 2 * share, 1e30, landed)
    step = 0.3 * jnp.min(jnp.min(lowest, axis=0, keepdims=True), axis=1, keepdims=True)
    for c, accel in enumerate((accel_x, accel_y)):
        speed = vel[c] + step * accel
        new_vel[c] = speed
        new_disp[c] = disp[c] + step * speed

    react_arrive()
    react_sum = step * jnp.sum(react_in[...], axis=0, keepdims=True)
    for c in range(3):
        piece = react_sum[:, c * share:(c + 1) * share]
        if c < 2:
            piece = piece + prior_sum[:, c * share:(c + 1) * share]
        new_imp[c:c + 1, :] = piece

    for copy in plane_copies + line_copies:
        copy.wait_send()

    @pl.when(has_up)
    def _():
        to_up.wait_send()

    @pl.when(has_down)
    def _():
        to_down.wait_send()

    @pl.when(has_left)
    def _():
        to_left.wait_send()

    @pl.when(has_right)
    def _():
        to_right.wait_send()

    early_drain()
    react_drain()


def write_kernel(vel, disp, imp, vel_out, disp_out, imp_out, sem):
    copies = [
        pltpu.make_async_copy(src, dst, sem.at[i])
        for i, (src, dst) in enumerate([(vel, vel_out), (disp, disp_out), (imp, imp_out)])
    ]
    for copy in copies:
        copy.start()
    for copy in copies:
        copy.wait()


def shards(n_gx, n_gy, node_disp, node_vel, node_mass, zone_mass, zone_energy, master_block, owner,
           pair_node, pair_segment, pair_side, pair_count):
    n = n_gx * n_gy
    rows, cols = node_mass.shape
    pairs = pair_node.shape[1]
    mnodes = master_block.shape[2]
    share = mnodes // n
    groups = mnodes // 128
    any_spec = pl.BlockSpec(memory_space=pltpu.HBM)
    vmem_spec = pl.BlockSpec(memory_space=pltpu.VMEM)
    smem = pltpu.SMEM
    vm = pltpu.VMEM
    dma = pltpu.SemaphoreType.DMA
    i32 = jnp.int32
    kept = pl.pallas_call(
        functools.partial(step_kernel, n_gx, n_gy),
        out_shape=(
            vm((2, rows, cols), F32), vm((2, rows, cols), F32), vm((3, share), F32),
        ),
        in_specs=[any_spec] * 11,
        out_specs=(vmem_spec,) * 3,
        scratch_shapes=[
            smem((1,), i32), smem((1,), i32),
            vm((2, rows, cols), F32), vm((2, rows, cols), F32), vm((rows, cols), F32), vm((rows, cols), F32),
            vm((rows, cols), F32), vm((1, 4, mnodes), BF16), vm((1, pairs), i32), vm((1, pairs), i32),
            vm((1, pairs), i32),
            vm((8, cols), F32), vm((8, cols), F32), vm((rows + 8, 128), F32), vm((rows + 8, 128), F32),
            vm((8, cols), F32), vm((8, cols), F32), vm((rows + 8, 128), F32), vm((rows + 8, 128), F32),
            vm((n_gx, 2 * groups, 128), BF16), vm((n_gy, 2 * groups, 128), BF16),
            vm((2 * groups, 128), F32),
            vm((cols, pairs), BF16), vm((128, pairs), BF16), vm((n, 2 * pairs), BF16),
            vm((n, 128), F32), vm((n, 128), F32), vm((n, 128), F32), vm((n, 128), F32),
            dma((11,)), dma((4,)), dma((4,)),
            dma((n_gx,)), dma((n_gx,)), dma((n_gy,)), dma((n_gy,)),
            dma((n,)), dma((n,)), dma((n,)), dma((n,)),
        ],
        compiler_params=pltpu.CompilerParams(collective_id=0, has_side_effects=True),
    )(owner, pair_count, node_disp, node_vel, node_mass, zone_mass, zone_energy, master_block,
      pair_node, pair_segment, pair_side)
    return pl.pallas_call(
        write_kernel,
        out_shape=tuple(jax.ShapeDtypeStruct(k.shape, k.dtype) for k in kept),
        in_specs=[vmem_spec] * 3,
        out_specs=(any_spec,) * 3,
        scratch_shapes=[dma((3,))],
    )(*[pltpu.with_memory_space_constraint(k, pltpu.VMEM) for k in kept])


def solution(mesh):
    in_specs = (
        P(None, "gx", "gy"), P(None, "gx", "gy"), P("gx", "gy"), P("gx", "gy"), P("gx", "gy"),
        P(("gx", "gy"), None, None), P(), P(("gx", "gy"), None), P(("gx", "gy"), None),
        P(("gx", "gy"), None), P(("gx", "gy")),
    )
    out_specs = (P(None, "gx", "gy"), P(None, "gx", "gy"), P(None, ("gx", "gy")))
    body = functools.partial(shards, mesh.shape["gx"], mesh.shape["gy"])
    return jax.shard_map(body, mesh=mesh, in_specs=in_specs, out_specs=out_specs, check_vma=False)
```

```python
import functools

import jax
import jax.numpy as jnp
from jax import lax
from jax.experimental import pallas as pl
from jax.experimental.pallas import tpu as pltpu
from jax.sharding import PartitionSpec as P

STIFFNESS = 10.0
GAP_SCALE = 0.05
MESH = pl.DeviceIdType.MESH
F32 = jnp.float32
BF16 = jnp.bfloat16


def two_parts(value):
    top = value.astype(BF16).astype(F32)
    return top, value - top


def dot_nt(left, right):
    return lax.dot_general(left, right, (((1,), (1,)), ((), ())), preferred_element_type=F32)


def rolled(value, shift, axis):
    return pltpu.roll(value, shift % value.shape[axis], axis)


def step_kernel(
    n_gx, n_gy,
    owner_in, count_in, disp_in, vel_in, mass_in, zmass_in, energy_in, block_in, node_in, seg_in, side_in,
    new_vel, new_disp, new_imp,
    owner_ref, count_ref, disp, vel, mass, zmass, energy, block, node, seg, side,
    up_pack, down_pack, left_pack, right_pack,
    from_down, from_up, from_right, from_left,
    plane_slots, line_slots, table,
    oh_col, oh_lo, oh_share, early, early_in, react, react_in,
    in_sem, halo_send, halo_recv,
    plane_send_sem, plane_recv_sem, line_send_sem, line_recv_sem,
    early_send_sem, early_recv_sem, react_send_sem, react_recv_sem,
):
    n = n_gx * n_gy
    mx, my = lax.axis_index("gx"), lax.axis_index("gy")
    me = mx * n_gy + my
    rows, cols = disp.shape[1], disp.shape[2]
    pairs = node.shape[1]
    mnodes = block.shape[2]
    share = mnodes // n
    groups = mnodes // 128

    loads = [
        pltpu.make_async_copy(src, dst, in_sem.at[i])
        for i, (src, dst) in enumerate(
            [(block_in, block), (node_in, node), (disp_in, disp), (seg_in, seg), (energy_in, energy),
             (zmass_in, zmass), (side_in, side), (owner_in, owner_ref), (count_in, count_ref), (mass_in, mass), (vel_in, vel)]
        )
    ]
    for load in loads:
        load.start()
    for ref in (from_down, from_up, from_right, from_left):
        ref[...] = jnp.zeros(ref.shape, F32)

    barrier = pltpu.get_barrier_semaphore()
    for d in range(1, n_gx):
        pl.semaphore_signal(barrier, inc=1, device_id=(lax.rem(mx + d, n_gx), my), device_id_type=MESH)
    for d in range(1, n_gy):
        pl.semaphore_signal(barrier, inc=1, device_id=(mx, lax.rem(my + d, n_gy)), device_id_type=MESH)

    for load in loads[:9]:
        load.wait()

    dx, dy = disp[0], disp[1]
    zload = energy[...] * zmass[...]
    sub = lax.broadcasted_iota(jnp.int32, (8, cols), 0)
    up_pack[...] = jnp.where(sub == 0, dx[:8], jnp.where(sub == 1, rolled(dy[:8], 1, 0), 0.0))
    tail = slice(rows - 8, rows)
    down_pack[...] = jnp.where(
        sub == 7, dx[tail],
        jnp.where(sub == 6, rolled(dy[tail], -1, 0), jnp.where(sub == 5, rolled(zload[tail], -2, 0), 0.0)),
    )
    own = block[0, 0:2].astype(F32)
    for c in range(2):
        for h in range(groups):
            table[c * groups + h:c * groups + h + 1, :] = own[c:c + 1, h * 128:(h + 1) * 128]
    plane_slots[mx] = table[...].astype(BF16)

    node_id = node[...]
    seg_id = seg[...]
    seg_next = seg_id + 1
    node_row, node_col = node_id // cols, node_id % cols
    oh_col[...] = (lax.broadcasted_iota(jnp.int32, (cols, pairs), 0) == node_col).astype(F32).astype(BF16)
    oh_lo[...] = (lax.broadcasted_iota(jnp.int32, (128, pairs), 0) == seg_id % 128).astype(F32).astype(BF16)
    share_iota = lax.broadcasted_iota(jnp.int32, (n, pairs), 0)
    oh_share[:, :pairs] = (share_iota == seg_id // share).astype(F32).astype(BF16)
    oh_share[:, pairs:] = (share_iota == seg_next // share).astype(F32).astype(BF16)
    row_mask = lax.broadcasted_iota(jnp.int32, (rows, pairs), 0) == node_row

    flat = disp[...].reshape(2 * rows, cols)
    flat_top, flat_low = two_parts(flat)
    looked = jnp.dot(
        jnp.concatenate([flat_top, flat_low], axis=0).astype(BF16), oh_col[...], preferred_element_type=F32
    )
    looked = looked[: 2 * rows] + looked[2 * rows:]
    slave_x = jnp.sum(jnp.where(row_mask, looked[:rows], 0.0), axis=0, keepdims=True)
    slave_y = jnp.sum(jnp.where(row_mask, looked[rows:], 0.0), axis=0, keepdims=True)

    owner = owner_ref[0]
    master_id = lax.broadcasted_iota(jnp.int32, (1, mnodes), 1)
    prior = jnp.where(owner == me, block[0, 2:4].astype(F32), 0.0)
    prior_mask = lax.broadcasted_iota(jnp.int32, (share, mnodes), 0) == master_id % share
    prior_cols = jnp.concatenate(
        [jnp.where(prior_mask, prior[0:1], 0.0), jnp.where(prior_mask, prior[1:2], 0.0),
         jnp.zeros((128 - 2 * share, mnodes), F32)], axis=0
    ).astype(BF16)
    prior_rows = (lax.broadcasted_iota(jnp.int32, (n, mnodes), 0) == master_id // share).astype(F32).astype(BF16)
    early[...] = dot_nt(prior_rows, prior_cols)

    pl.semaphore_wait(barrier, n_gx + n_gy - 2)

    plane_copies = []
    for d in range(1, n_gx):
        plane_copies.append(pltpu.make_async_remote_copy(
            src_ref=plane_slots.at[mx], dst_ref=plane_slots.at[mx],
            send_sem=plane_send_sem.at[d], recv_sem=plane_recv_sem.at[d],
            device_id=(lax.rem(mx + d, n_gx), my), device_id_type=MESH))
        plane_copies[-1].start()

    def halo(src, dst, slot, device):
        return pltpu.make_async_remote_copy(
            src_ref=src, dst_ref=dst, send_sem=halo_send.at[slot], recv_sem=halo_recv.at[slot],
            device_id=device, device_id_type=MESH)

    to_up = halo(up_pack, from_down, 0, (jnp.maximum(mx - 1, 0), my))
    to_down = halo(down_pack, from_up, 1, (jnp.minimum(mx + 1, n_gx - 1), my))
    to_left = halo(left_pack, from_right, 2, (mx, jnp.maximum(my - 1, 0)))
    to_right = halo(right_pack, from_left, 3, (mx, jnp.minimum(my + 1, n_gy - 1)))
    has_up, has_down = mx > 0, mx < n_gx - 1
    has_left, has_right = my > 0, my < n_gy - 1

    @pl.when(has_up)
    def _():
        to_up.start()

    @pl.when(has_down)
    def _():
        to_down.start()

    for d in range(1, n_gx):
        pltpu.make_async_remote_copy(
            src_ref=plane_slots.at[mx], dst_ref=plane_slots.at[lax.rem(mx + n_gx - d, n_gx)],
            send_sem=plane_send_sem.at[d], recv_sem=plane_recv_sem.at[d],
            device_id=(lax.rem(mx + d, n_gx), my), device_id_type=MESH).wait_recv()

    line_slots[my] = plane_slots[owner // n_gy]
    line_copies = []
    for d in range(1, n_gy):
        line_copies.append(pltpu.make_async_remote_copy(
            src_ref=line_slots.at[my], dst_ref=line_slots.at[my],
            send_sem=line_send_sem.at[d], recv_sem=line_recv_sem.at[d],
            device_id=(mx, lax.rem(my + d, n_gy)), device_id_type=MESH))
        line_copies[-1].start()

    @pl.when(has_down)
    def _():
        to_up.wait_recv()

    @pl.when(has_up)
    def _():
        to_down.wait_recv()

    below, above = from_down[...], from_up[...]
    ext_x = jnp.concatenate([dx, jnp.where(sub < 4, below, above)], axis=0)
    ext_y = jnp.concatenate([dy, jnp.where(sub < 4, rolled(below, -1, 0), rolled(above, 1, 0))], axis=0)
    ext_l = jnp.concatenate([zload, rolled(above, 2, 0)], axis=0)
    lane = lax.broadcasted_iota(jnp.int32, (rows + 8, 128), 1)
    last = slice(cols - 128, cols)
    left_pack[...] = jnp.where(lane == 0, ext_x[:, :128], jnp.where(lane == 1, rolled(ext_y[:, :128], 1, 1), 0.0))
    right_pack[...] = jnp.where(
        lane == 127, ext_x[:, last],
        jnp.where(lane == 126, rolled(ext_y[:, last], -1, 1),
                  jnp.where(lane == 125, rolled(ext_l[:, last], -2, 1), 0.0)),
    )

    @pl.when(has_left)
    def _():
        to_left.start()

    @pl.when(has_right)
    def _():
        to_right.start()

    @pl.when(has_right)
    def _():
        to_left.wait_recv()

    @pl.when(has_left)
    def _():
        to_right.wait_recv()

    right, left = from_right[...], from_left[...]
    ext_x = jnp.concatenate([ext_x, jnp.where(lane < 64, right, left)], axis=1)
    ext_y = jnp.concatenate([ext_y, jnp.where(lane < 64, rolled(right, -1, 1), rolled(left, 1, 1))], axis=1)
    ext_l = jnp.concatenate([ext_l, rolled(left, 2, 1)], axis=1)
    ext_shape = ext_x.shape
    zone_row = lax.broadcasted_iota(jnp.int32, ext_shape, 0)
    zone_row = jnp.where(zone_row == ext_shape[0] - 1, -1, zone_row) + mx * rows
    zone_col = lax.broadcasted_iota(jnp.int32, ext_shape, 1)
    zone_col = jnp.where(zone_col == ext_shape[1] - 1, -1, zone_col) + my * cols
    live = (zone_row >= 0) & (zone_row < n_gx * rows - 1) & (zone_col >= 0) & (zone_col < n_gy * cols - 1)
    b_x, b_y = rolled(ext_x, -1, 0), rolled(ext_y, -1, 0)
    c_x, c_y = rolled(b_x, -1, 1), rolled(b_y, -1, 1)
    e_x, e_y = rolled(ext_x, -1, 1), rolled(ext_y, -1, 1)
    first_dx, first_dy = 1.0 + c_x - ext_x, 1.0 + c_y - ext_y
    second_dx, second_dy = -1.0 + e_x - b_x, 1.0 + e_y - b_y
    area = jnp.where(live, 0.5 * (first_dx * second_dy - second_dx * first_dy), 1.0)
    half_press = jnp.where(live, 0.2 * ext_l / area, 0.0)
    fa_x, fa_y = -half_press * second_dy, half_press * second_dx
    fb_x, fb_y = half_press * first_dy, -half_press * first_dx

    def gather_force(on_a, on_b):
        total = on_a + rolled(on_b - rolled(on_a, 1, 1), 1, 0) - rolled(on_b, 1, 1)
        return total[:rows, :cols]

    force_x, force_y = gather_force(fa_x, fb_x), gather_force(fa_y, fb_y)
    ratio = jnp.where(
        live[:rows, :cols], jnp.sqrt(area[:rows, :cols]) / jnp.sqrt(0.56 * energy[...]), 1e30
    )
    smallest = jnp.min(jnp.min(ratio, axis=0, keepdims=True), axis=1, keepdims=True)
    early_lane = lax.broadcasted_iota(jnp.int32, (n, 128), 1)
    early[...] = jnp.where(early_lane < 2 * share, early[...], smallest)

    for d in range(1, n_gy):
        pltpu.make_async_remote_copy(
            src_ref=line_slots.at[my], dst_ref=line_slots.at[lax.rem(my + n_gy - d, n_gy)],
            send_sem=line_send_sem.at[d], recv_sem=line_recv_sem.at[d],
            device_id=(mx, lax.rem(my + d, n_gy)), device_id_type=MESH).wait_recv()

    def exchange(sent, landed, send_sem, recv_sem):
        def copy(d, slot):
            target = lax.rem(me + d, n)
            return pltpu.make_async_remote_copy(
                src_ref=sent.at[pl.ds(target, 1)], dst_ref=landed.at[pl.ds(slot, 1)],
                send_sem=send_sem.at[d], recv_sem=recv_sem.at[d],
                device_id=(target // n_gy, lax.rem(target, n_gy)), device_id_type=MESH)

        def start():
            landed[pl.ds(me, 1), :] = sent[pl.ds(me, 1), :]

            def body(d, carry):
                copy(d, me).start()
                return carry
            lax.fori_loop(1, n, body, 0, unroll=n <= 64)

        def arrive():
            def body(d, carry):
                copy(d, lax.rem(me + n - d, n)).wait_recv()
                return carry
            lax.fori_loop(1, n, body, 0, unroll=n <= 64)

        def drain():
            def body(d, carry):
                copy(d, me).wait_send()
                return carry
            lax.fori_loop(1, n, body, 0, unroll=n <= 64)
        return start, arrive, drain

    early_start, early_arrive, early_drain = exchange(early, early_in, early_send_sem, early_recv_sem)
    react_start, react_arrive, react_drain = exchange(react, react_in, react_send_sem, react_recv_sem)
    early_start()

    coords = line_slots[lax.rem(owner, n_gy)].astype(F32)
    shifted = rolled(coords, -1, 1)
    last_lane = lax.broadcasted_iota(jnp.int32, coords.shape, 1) == 127
    shifted = jnp.where(last_lane, rolled(shifted, -1, 0), shifted)
    looked = jnp.dot(
        jnp.concatenate([coords, shifted], axis=0).astype(BF16), oh_lo[...], preferred_element_type=F32
    )
    group_mask = lax.broadcasted_iota(jnp.int32, (groups, pairs), 0) == seg_id // 128
    start_x, start_y, end_x, end_y = [
        jnp.sum(jnp.where(group_mask, looked[q * groups:(q + 1) * groups], 0.0), axis=0, keepdims=True)
        for q in range(4)
    ]
    live_mask = lax.broadcasted_iota(jnp.int32, (1, pairs), 1) < count_ref[0]
    rel_x, rel_y = slave_x - start_x + 0.5, slave_y - start_y
    along_x, along_y = 1.0 + end_x - start_x, end_y - start_y
    along_sq = along_x * along_x + along_y * along_y
    length = jnp.sqrt(along_sq)
    fraction = (rel_x * along_x + rel_y * along_y) / along_sq
    normal_x, normal_y = -along_y / length, along_x / length
    gap_size = normal_x * rel_x + normal_y * rel_y
    side_sign = 1.0 - 2.0 * side[...].astype(F32)
    pressed = -side_sign * gap_size / GAP_SCALE
    soft = jnp.maximum(pressed, 0.0) + jnp.log1p(jnp.exp(-jnp.abs(pressed)))
    magnitude = jnp.where(live_mask, STIFFNESS * GAP_SCALE * soft, 0.0)
    push_x, push_y = magnitude * side_sign * normal_x, magnitude * side_sign * normal_y
    terms = (-push_x, -push_y, magnitude)
    firsts = [two_parts((1.0 - fraction) * t) for t in terms]
    seconds = [two_parts(fraction * t) for t in terms]
    lane_iota = lax.broadcasted_iota(jnp.int32, (share, pairs), 0)
    total = None
    for values, ids, half in ((firsts, seg_id, 0), (seconds, seg_next, 1)):
        lane_mask = lane_iota == ids % share
        for part in range(2):
            spread = jnp.concatenate(
                [jnp.where(lane_mask, values[c][part], 0.0) for c in range(3)]
                + [jnp.zeros((128 - 3 * share, pairs), F32)], axis=0
            ).astype(BF16)
            piece = dot_nt(oh_share[:, half * pairs:(half + 1) * pairs], spread)
            total = piece if total is None else total + piece
    react[...] = total
    react_start()

    (px_top, px_low), (py_top, py_low) = two_parts(push_x), two_parts(push_y)
    placed = jnp.concatenate(
        [jnp.where(row_mask, v, 0.0).astype(BF16) for v in (px_top, py_top, px_low, py_low)], axis=0
    )
    pushed = dot_nt(placed, oh_col[...])
    pushed = pushed[: 2 * rows] + pushed[2 * rows:]
    loads[9].wait()
    loads[10].wait()
    inv_mass = 1.0 / mass[...]
    accel_x = (force_x + pushed[:rows]) * inv_mass
    accel_y = (force_y + pushed[rows:]) * inv_mass

    early_arrive()
    landed = early_in[...]
    prior_sum = jnp.sum(landed, axis=0, keepdims=True)
    lowest = jnp.where(early_lane < 2 * share, 1e30, landed)
    step = 0.3 * jnp.min(jnp.min(lowest, axis=0, keepdims=True), axis=1, keepdims=True)
    for c, accel in enumerate((accel_x, accel_y)):
        speed = vel[c] + step * accel
        new_vel[c] = speed
        new_disp[c] = disp[c] + step * speed

    react_arrive()
    react_sum = step * jnp.sum(react_in[...], axis=0, keepdims=True)
    for c in range(3):
        piece = react_sum[:, c * share:(c + 1) * share]
        if c < 2:
            piece = piece + prior_sum[:, c * share:(c + 1) * share]
        new_imp[c:c + 1, :] = piece

    for copy in plane_copies + line_copies:
        copy.wait_send()

    @pl.when(has_up)
    def _():
        to_up.wait_send()

    @pl.when(has_down)
    def _():
        to_down.wait_send()

    @pl.when(has_left)
    def _():
        to_left.wait_send()

    @pl.when(has_right)
    def _():
        to_right.wait_send()

    early_drain()
    react_drain()


def write_kernel(vel, disp, imp, vel_out, disp_out, imp_out, sem):
    copies = [
        pltpu.make_async_copy(src, dst, sem.at[i])
        for i, (src, dst) in enumerate([(vel, vel_out), (disp, disp_out), (imp, imp_out)])
    ]
    for copy in copies:
        copy.start()
    for copy in copies:
        copy.wait()


def shards(n_gx, n_gy, node_disp, node_vel, node_mass, zone_mass, zone_energy, master_block, owner,
           pair_node, pair_segment, pair_side, pair_count):
    n = n_gx * n_gy
    rows, cols = node_mass.shape
    pairs = pair_node.shape[1]
    mnodes = master_block.shape[2]
    share = mnodes // n
    groups = mnodes // 128
    any_spec = pl.BlockSpec(memory_space=pltpu.HBM)
    vmem_spec = pl.BlockSpec(memory_space=pltpu.VMEM)
    smem = pltpu.SMEM
    vm = pltpu.VMEM
    dma = pltpu.SemaphoreType.DMA
    i32 = jnp.int32
    kept = pl.pallas_call(
        functools.partial(step_kernel, n_gx, n_gy),
        out_shape=(
            vm((2, rows, cols), F32), vm((2, rows, cols), F32), vm((3, share), F32),
        ),
        in_specs=[any_spec] * 11,
        out_specs=(vmem_spec,) * 3,
        scratch_shapes=[
            smem((1,), i32), smem((1,), i32),
            vm((2, rows, cols), F32), vm((2, rows, cols), F32), vm((rows, cols), F32), vm((rows, cols), F32),
            vm((rows, cols), F32), vm((1, 4, mnodes), BF16), vm((1, pairs), i32), vm((1, pairs), i32),
            vm((1, pairs), i32),
            vm((8, cols), F32), vm((8, cols), F32), vm((rows + 8, 128), F32), vm((rows + 8, 128), F32),
            vm((8, cols), F32), vm((8, cols), F32), vm((rows + 8, 128), F32), vm((rows + 8, 128), F32),
            vm((n_gx, 2 * groups, 128), BF16), vm((n_gy, 2 * groups, 128), BF16),
            vm((2 * groups, 128), F32),
            vm((cols, pairs), BF16), vm((128, pairs), BF16), vm((n, 2 * pairs), BF16),
            vm((n, 128), F32), vm((n, 128), F32), vm((n, 128), F32), vm((n, 128), F32),
            dma((11,)), dma((4,)), dma((4,)),
            dma((n_gx,)), dma((n_gx,)), dma((n_gy,)), dma((n_gy,)),
            dma((n,)), dma((n,)), dma((n,)), dma((n,)),
        ],
        compiler_params=pltpu.CompilerParams(collective_id=0, has_side_effects=True),
    )(owner, pair_count, node_disp, node_vel, node_mass, zone_mass, zone_energy, master_block,
      pair_node, pair_segment, pair_side)
    return pl.pallas_call(
        write_kernel,
        out_shape=tuple(jax.ShapeDtypeStruct(k.shape, k.dtype) for k in kept),
        in_specs=[vmem_spec] * 3,
        out_specs=(any_spec,) * 3,
        scratch_shapes=[dma((3,))],
    )(*[pltpu.with_memory_space_constraint(k, pltpu.VMEM) for k in kept])


def solution(mesh):
    in_specs = (
        P(None, "gx", "gy"), P(None, "gx", "gy"), P("gx", "gy"), P("gx", "gy"), P("gx", "gy"),
        P(("gx", "gy"), None, None), P(), P(("gx", "gy"), None), P(("gx", "gy"), None),
        P(("gx", "gy"), None), P(("gx", "gy")),
    )
    out_specs = (P(None, "gx", "gy"), P(None, "gx", "gy"), P(None, ("gx", "gy")))
    body = functools.partial(shards, mesh.shape["gx"], mesh.shape["gy"])
    return jax.shard_map(body, mesh=mesh, in_specs=in_specs, out_specs=out_specs, check_vma=False)
```
